32 devices in a mesh: chan: 4 (over y, x), slab: 8 (over z, core).
Axes of the slice: x: 2, y: 2, z: 4, core: 2. Of those that a mesh axis runs over, the one named last changes fastest.
Arguments:
- flux: float32 [4, 512, 128], P('chan', 'slab'), may hold values from -6 to 6
- offsets: int32 [512, 128], P('slab'), may hold values from 0 to 8191
- counts: int32 [512], P('slab'), may hold values from 96 to 128
- dest_owner: int32 [512, 1], P('slab'), may hold values from 0 to 7; in each aligned block of 64 rows (0 to 63, 64 to 127, ...) at most 16 rows name the same one
- dest_tile: int32 [512], P('slab'), may hold values from 0 to 255
- dirty: float32 [4, 4096, 4096], P('chan', 'slab'), may hold values from -60 to 60
- psf_real: float32 [4, 8192, 8192], P('chan', None, 'slab'), may hold values from -96 to 96
- psf_imag: float32 [4, 8192, 8192], P('chan', None, 'slab'), may hold values from -96 to 96
Outputs:
- residual: float32 [4, 4096, 4096], P('chan', 'slab')
- rms_values: float32 [4], replicated
- peak_values: float32 [4], replicated
The draws below stay inside these ranges and needn't reach their ends.
Inputs may be any that keep to these rules, and one draw needn't show every extreme that they name: `dest_owner`: among the 64 blocks of one device (aligned blocks of rows) at most 16 name the same owner, a bound that some device reaches. `counts`: slots at or beyond a block's count hold no component.
All inputs are finite; a program needn't handle non-finite values.
Results may differ from the reference program's by a relative error of at most 0.00005.
Values sent between devices are 32-bit elements; how exact they have to be, the bound alone decides.
A program may use at most 384 MiB of HBM per device.

```python
import math
import jax
import jax.numpy as jnp
import numpy as np
from jax import lax

IMG = 4096
COMP = 128
TILE_R = 64
TILE_C = 128
BLK_DEV = 64
PAD = 8192
SEND = 16
TILES_OWN = 256
CHANNELS = 4
BLOCKS = 512
N_SLAB = 8


def draw_dirty(key, part):
    key_base = jax.random.fold_in(key, 11)
    key_cols = jax.random.fold_in(key, 12)
    row_frac = jnp.arange(IMG, dtype=jnp.float32)[:, None] / IMG
    col_frac = jax.random.uniform(key_cols, (1, IMG), jnp.float32)
    base_noise = jnp.clip(jax.random.normal(key_base, (CHANNELS, IMG, IMG), jnp.float32), -6.0, 6.0)
    return 0.3 * base_noise * 10.0 ** row_frac * 10.0 ** (0.5 * col_frac)


def set_ends(result, rng, low, top_value):
    shape = result.shape
    place = [jax.random.randint(jax.random.fold_in(rng, axis), (), 0, shape[axis]) for axis in range(len(shape))]
    result = result.at[tuple(place)].set(low)
    longest = shape.index(max(shape))
    place[longest] = (place[longest] + 1) % shape[longest]
    return result.at[tuple(place)].set(top_value)


def block_levels(stream_key, dims, shards, smallest, top_value):
    factor_of, own = 1.0, jax.random.fold_in(stream_key, 6)
    for position, shards_of in shards:
        draws = jnp.exp(jax.random.uniform(jax.random.fold_in(own, position), (shards_of,), jnp.float32, smallest / len(shards), top_value / len(shards)))
        factor_of = factor_of * jnp.repeat(draws, dims[position] // shards_of).reshape([-1 if axis == position else 1 for axis in range(len(dims))])
    return factor_of


def deal_out(key, own, number, rows, number_of, top, reach, slope):
    order = jax.random.permutation(key, number_of)
    heavy_load, usual = load_shares(number_of, rows * top, reach, slope, True), load_shares(number_of, rows * top, reach, slope, False)
    places = jnp.arange(number_of)

    def named(tallies, rotation):
        used = int((tallies > 0).sum())
        fixed = max(1, used // 4)
        passed = fixed + (places - fixed + rotation * (used - fixed)) % max(1, number_of - fixed)
        return jnp.zeros((number_of,), jnp.int32).at[order[jnp.where(places < fixed, places, passed)]].set(jnp.asarray(tallies, jnp.int32))

    tallies = jnp.where(number % 4 == 0, named(heavy_load, number // 4), named(usual, number - number // 4 - 1))
    mixed = jax.random.permutation(jax.random.fold_in(own, 3), number_of)
    donor, receiver = mixed[0:number_of // 2 * 2:2], mixed[1:number_of // 2 * 2:2]
    room = jnp.minimum(tallies[donor] - 1, reach - tallies[receiver]) // 2
    room = jnp.where((donor == order[0]) | (receiver == order[0]) | (tallies[receiver] == 0), 0, jnp.maximum(room, 0))
    passed = jax.random.randint(jax.random.fold_in(own, 4), (number_of // 2,), 0, 1 << 20) % (room + 1)
    tallies = tallies.at[donor].add(-passed).at[receiver].add(passed)
    items = jnp.searchsorted(jnp.cumsum(tallies), jnp.arange(rows * top), side="right").astype(jnp.int32)
    listing = items.reshape(top, rows).T
    listing = listing[jax.random.permutation(jax.random.fold_in(own, 1), rows)]
    rotation = jax.random.randint(jax.random.fold_in(own, 2), (rows, 1), 0, top)
    return jnp.take_along_axis(listing, (jnp.arange(top)[None, :] + rotation) % top, axis=1)


def load_shares(amount, total, most, lean, full):
    portions = [(1 << 20) // math.isqrt(standing ** lean) + 1 for standing in range(1, amount + 1)]
    largest = most if full else min(most, max(-(-total // amount), total * portions[0] // sum(portions)))
    least = 1 if total - largest >= amount - 1 else 0
    holding, spare = [largest] + [least] * (amount - 1), total - largest - least * (amount - 1)
    while spare > 0:
        movable = [i for i in range(1, amount) if holding[i] < largest] or [i for i in range(1, amount) if holding[i] < most]
        whole, remaining = sum([portions[i] for i in movable]), spare
        for i in movable:
            addition = min(most - holding[i], max(1, remaining * portions[i] // whole), spare)
            holding[i] = holding[i] + addition
            spare = spare - addition
    return np.array(holding)


def noise(key, dims, spread, bound, shards=(), kind=jnp.bfloat16):
    result = jax.random.normal(key, dims, jnp.float32) * spread
    if len(shards) > 0:
        result = block_levels(key, dims, shards, -0.22, 0.18) * result
    return jnp.clip(result, min=-bound, max=bound).astype(kind)


def setup_inputs(seed: int = 0) -> dict:
    streams_of = jax.random.split(jax.random.key(seed), 9)
    flux = noise(streams_of[0], (CHANNELS, BLOCKS, COMP), 1.0, 6.0, ((0, 4), (1, 8)), jnp.float32)
    offsets = set_ends(jax.random.randint(streams_of[1], (BLOCKS, COMP), 0, TILE_R * TILE_C), jax.random.fold_in(streams_of[1], 1), 0, (TILE_R * TILE_C) - 1).astype(jnp.int32)
    counts = set_ends(jax.random.randint(streams_of[2], (BLOCKS,), COMP * 3 // 4, COMP + 1), jax.random.fold_in(streams_of[2], 1), COMP * 3 // 4, COMP).astype(jnp.int32)
    dest_owner_keys = jax.random.split(jax.random.fold_in(streams_of[3], 1), BLOCKS // BLK_DEV)
    dest_owner_turns = jax.random.permutation(jax.random.fold_in(streams_of[3], 3), BLOCKS // BLK_DEV)
    dest_owner = jax.vmap(lambda own, number: deal_out(jax.random.fold_in(streams_of[3], 2), own, number, BLK_DEV, N_SLAB, 1, SEND, 2))(dest_owner_keys, dest_owner_turns).reshape((BLOCKS, 1))
    dest_tile = set_ends(jax.random.randint(streams_of[4], (BLOCKS,), 0, TILES_OWN), jax.random.fold_in(streams_of[4], 1), 0, TILES_OWN - 1).astype(jnp.int32)
    dirty = draw_dirty(jax.random.fold_in(streams_of[8], 71), 0)
    psf_real = noise(streams_of[6], (CHANNELS, PAD, PAD), (PAD // 512), 96.0, ((0, 4), (2, 8)), jnp.float32)
    psf_imag = noise(streams_of[7], (CHANNELS, PAD, PAD), (PAD // 512), 96.0, ((0, 4), (2, 8)), jnp.float32)
    return {"flux": flux, "offsets": offsets, "counts": counts, "dest_owner": dest_owner, "dest_tile": dest_tile, "dirty": dirty, "psf_real": psf_real, "psf_imag": psf_imag}


def reference(flux, offsets, counts, dest_owner, dest_tile, dirty, psf_real, psf_imag):
    rows_dev = IMG // N_SLAB
    across = IMG // TILE_C
    tile_row = dest_tile // across
    tile_col = dest_tile % across
    owner_ids = dest_owner[:, 0]
    pixels = ((owner_ids[:, None] * rows_dev + tile_row[:, None] * TILE_R + offsets // TILE_C) * IMG + tile_col[:, None] * TILE_C + offsets % TILE_C).reshape(-1).astype(jnp.int32)
    live_mask = jnp.arange(COMP, dtype=jnp.int32)[None, :] < counts[:, None]
    weights = jnp.where(live_mask[None], flux, jnp.zeros_like(flux)).reshape(CHANNELS, -1)

    def one_channel(members):
        weight, dirty_part, spec_real, spec_imag = members
        model_image = jnp.zeros((IMG * IMG,), flux.dtype).at[pixels].add(weight).reshape(IMG, IMG)
        spectrum = jnp.fft.fft2(model_image, s=(PAD, PAD))
        convolved = jnp.fft.ifft2(spectrum * lax.complex(spec_real, spec_imag))
        residual = dirty_part - jnp.real(convolved[:IMG, :IMG])
        return (residual, jnp.sqrt(jnp.mean(residual * residual)), jnp.max(jnp.abs(residual)))
    residual, rms_values, peak_values = lax.map(one_channel, (weights, dirty, psf_real, psf_imag))
    return (residual, rms_values, peak_values)
```

```python
import math

import jax
import jax.numpy as jnp
from jax import lax
from jax.experimental import pallas as pl
from jax.experimental.pallas import tpu as pltpu
from jax.sharding import PartitionSpec as P


TILE_R = 64
TILE_C = 128
LANES = 128
PAINT = 32
BATCH = 64
NEAR = 16
PITCH = 72
ODD = 65
F32 = jnp.float32
BF16 = jnp.bfloat16
VMEM_LIMIT = 64 * 1024 * 1024 - 128 * 1024


def unit(turns, length, sign):
    angles = (turns % length).astype(F32) * (2.0 * math.pi / length)
    return jnp.cos(angles), sign * jnp.sin(angles)


def product(one, two):
    return one[0] * two[0] - one[1] * two[1], one[0] * two[1] + one[1] * two[0]


def high_part(values):
    return lax.reduce_precision(values, 8, 7)


def left_parts(values):
    high = high_part(values)
    low = values - high
    return jnp.concatenate([high, high, low], axis=-1).astype(BF16)


def right_parts(values):
    high = values.astype(BF16)
    low = (values - high.astype(F32)).astype(BF16)
    return jnp.concatenate([high, low, high], axis=0)


def dot(first, second):
    return lax.dot_general(
        first, second, (((1,), (0,)), ((), ())), preferred_element_type=F32
    )


def combine(both, conj):
    count = both.shape[0] // 2
    width = both.shape[1] // 2
    cos_re, cos_im = both[:count, :width], both[:count, width:]
    sin_re, sin_im = both[count:, :width], both[count:, width:]
    if conj:
        return cos_re + sin_im, cos_im - sin_re
    return cos_re - sin_im, cos_im + sin_re


def params():
    return pltpu.CompilerParams(
        dimension_semantics=("arbitrary",), vmem_limit_bytes=VMEM_LIMIT
    )


def cost(flops, moved):
    return pl.CostEstimate(flops=int(flops), bytes_accessed=int(moved), transcendentals=0)


def tile_kernel(rows_ref, cols_ref, amounts_ref, tiles_ref):
    slots = rows_ref.shape[-1]
    row_iota = lax.broadcasted_iota(jnp.int32, (TILE_R, slots), 0)
    col_iota = lax.broadcasted_iota(jnp.int32, (TILE_C, slots), 0)
    for index in range(PAINT):
        amounts = amounts_ref[index]
        high = amounts.astype(BF16).astype(F32)
        low = amounts - high
        here = row_iota == rows_ref[index]
        spread = jnp.concatenate(
            [jnp.where(here, high, 0.0), jnp.where(here, low, 0.0)], axis=0
        ).astype(BF16)
        marks = jnp.where(col_iota == cols_ref[index], 1.0, 0.0).astype(BF16)
        both = lax.dot_general(
            spread, marks, (((1,), (1,)), ((), ())), preferred_element_type=F32
        )
        tile = both[:TILE_R] + both[TILE_R:]
        tile_high = tile.astype(BF16)
        tile_low = (tile - tile_high.astype(F32)).astype(BF16)
        place = pl.ds(index * TILE_R, TILE_R)
        tiles_ref[place, :TILE_C] = tile_high
        tiles_ref[place, TILE_C:] = tile_low


def make_tiles(rows, cols, amounts):
    blocks, _, slots = rows.shape
    part = pl.BlockSpec((PAINT, 1, slots), lambda step: (step, 0, 0))
    return pl.pallas_call(
        tile_kernel,
        out_shape=jax.ShapeDtypeStruct((blocks * TILE_R, 2 * TILE_C), BF16),
        grid=(blocks // PAINT,),
        in_specs=[part, part, part],
        out_specs=pl.BlockSpec((PAINT * TILE_R, 2 * TILE_C), lambda step: (step, 0)),
        compiler_params=params(),
        cost_estimate=cost(blocks * 4e7, blocks * 4e4),
    )(rows, cols, amounts)


def row_kernel(bands, tile_cols, tiles_ref, basis_ref, turn_ref, out_ref):
    blocks = bands.shape[0]
    out_ref[...] = jnp.zeros_like(out_ref)
    size = BATCH * TILE_R

    def step_of(step, carry):
        start = pl.multiple_of(step * size, size)
        tiles = tiles_ref[pl.ds(start, size), :]
        values = dot(jnp.concatenate([tiles, tiles[:, :TILE_C]], axis=1), basis_ref[...])
        for index in range(BATCH):
            block = step * BATCH + index
            turn = turn_ref[pl.ds(tile_cols[block], 1), :]
            turn_re, turn_im = turn[:, :LANES], turn[:, LANES:]
            part = values[index * TILE_R : (index + 1) * TILE_R]
            part_re, part_im = part[:, :LANES], part[:, LANES:]
            place = pl.ds(pl.multiple_of(bands[block] * PITCH, 8), TILE_R)
            out_ref[0, place, :] += part_re * turn_re - part_im * turn_im
            out_ref[1, place, :] += part_re * turn_im + part_im * turn_re
        return carry

    lax.fori_loop(0, blocks // BATCH, step_of, 0)


def row_transform(bands, tile_cols, tiles, basis, turns, width, first, count):
    blocks = bands.shape[0]
    across = turns.shape[0]
    height = width // TILE_R * PITCH
    return pl.pallas_call(
        row_kernel,
        out_shape=jax.ShapeDtypeStruct((2, height, count * LANES), F32),
        grid_spec=pltpu.PrefetchScalarGridSpec(
            num_scalar_prefetch=2,
            grid=(count,),
            in_specs=[
                pl.BlockSpec(
                    tiles.shape, lambda step, *_: (0, 0), pipeline_mode=pl.Buffered(1)
                ),
                pl.BlockSpec((3 * TILE_C, 2 * LANES), lambda step, *_: (0, step + first)),
                pl.BlockSpec((across, 2 * LANES), lambda step, *_: (0, step + first)),
            ],
            out_specs=pl.BlockSpec((2, height, LANES), lambda step, *_: (0, 0, step)),
        ),
        compiler_params=params(),
        cost_estimate=cost(blocks * count * 3e7, width * count * 1024),
    )(bands, tile_cols, tiles, basis, turns)


def paired(re, im):
    rows, cols = re.shape
    both = jnp.stack(
        [re.reshape(rows, cols // LANES, LANES), im.reshape(rows, cols // LANES, LANES)], axis=2
    )
    return both.reshape(rows, 2 * cols)


def row_tables(first_col, col_count, length, across):
    cols = first_col + jnp.arange(col_count, dtype=jnp.int32)[None, :]
    fine = paired(*unit(jnp.arange(TILE_C, dtype=jnp.int32)[:, None] * cols, length, -1.0))
    high = high_part(fine)
    basis = jnp.concatenate([high, high, fine - high], axis=0).astype(BF16)
    points = jnp.arange(across, dtype=jnp.int32)[:, None] * TILE_C
    return basis, paired(*unit(points * cols, length, -1.0))


def paint_kernel(starts, tile_cols, rows_ref, cols_ref, amounts_ref, image_ref):
    step = pl.program_id(0)
    image_ref[...] = jnp.zeros_like(image_ref)
    slots = rows_ref.shape[-1]
    row_iota = lax.broadcasted_iota(jnp.int32, (TILE_R, slots), 0)
    col_iota = lax.broadcasted_iota(jnp.int32, (TILE_C, slots), 0)

    def add_block(index, carry):
        spread = jnp.where(row_iota == rows_ref[index], amounts_ref[index], 0.0)
        marks = (col_iota == cols_ref[index]).astype(F32)
        tile = lax.dot_general(
            spread,
            marks,
            (((1,), (1,)), ((), ())),
            precision=lax.Precision.HIGHEST,
            preferred_element_type=F32,
        )
        place = pl.ds(pl.multiple_of(tile_cols[index] * TILE_C, TILE_C), TILE_C)
        image_ref[:, place] = image_ref[:, place] + tile
        return carry

    lax.fori_loop(starts[step], starts[step + 1], add_block, 0)


def dense_rows(bands, tile_cols, rows, cols, amounts, width, first_col, col_count, length):
    blocks, _, slots = rows.shape
    band_count = width // TILE_R
    order = jnp.argsort(bands)
    edges = jnp.arange(band_count + 1, dtype=jnp.int32)
    starts = jnp.sum((bands[None, :] < edges[:, None]).astype(jnp.int32), axis=1)
    whole = pl.BlockSpec((blocks, 1, slots), lambda step, *_: (0, 0, 0))
    image = pl.pallas_call(
        paint_kernel,
        out_shape=jax.ShapeDtypeStruct((width, width), F32),
        grid_spec=pltpu.PrefetchScalarGridSpec(
            num_scalar_prefetch=2,
            grid=(band_count,),
            in_specs=[whole, whole, whole],
            out_specs=pl.BlockSpec((TILE_R, width), lambda step, *_: (step, 0)),
        ),
    )(starts, tile_cols[order], rows[order], cols[order], amounts[order])
    ids = first_col + jnp.arange(col_count, dtype=jnp.int32)[None, :]
    low_len = 2 ** ((width.bit_length() - 1) // 2)
    low = unit(jnp.arange(low_len, dtype=jnp.int32)[:, None] * ids, length, -1.0)
    high = unit(
        jnp.arange(width // low_len, dtype=jnp.int32)[:, None] * low_len * ids, length, -1.0
    )
    table = product([part[:, None] for part in high], [part[None] for part in low])
    table = [part.reshape(width, col_count) for part in table]
    made = jnp.stack([jnp.dot(image, part, precision=lax.Precision.HIGH) for part in table])
    made = made.reshape(2, band_count, TILE_R, col_count)
    made = jnp.pad(made, ((0, 0), (0, 0), (0, PITCH - TILE_R), (0, 0)))
    return made.reshape(2, band_count * PITCH, col_count)


def both_parts(ref, rows):
    return right_parts(jnp.concatenate([ref[0, rows, :], ref[1, rows, :]], axis=1))


def column_kernel(plan, owners, pieces, first, spread_ref, psf_re, psf_im, outer_ref, inner_ref, back_ref, *rest):
    outs, (work, psf, arrived) = rest[: len(plan)], rest[len(plan) :]
    inner = TILE_R
    half = spread_ref.shape[1] // PITCH
    outer = 2 * half
    step_id = pl.program_id(0)
    steps = pl.num_programs(0)

    def copies(step):
        slot = step % 2
        cols = pl.ds(pl.multiple_of((first + step) * LANES, LANES), LANES)
        return [
            pltpu.make_async_copy(
                source.at[:, :, cols],
                psf.at[slot, part, :, pl.ds(0, outer), :],
                arrived.at[slot, part],
            )
            for part, source in enumerate((psf_re, psf_im))
        ]

    @pl.when(step_id == 0)
    def _():
        for copy in copies(step_id):
            copy.start()

    @pl.when(step_id + 1 < steps)
    def _():
        for copy in copies(step_id + 1):
            copy.start()

    def forward(step, carry):
        for index in range(NEAR):
            place = step * NEAR + index
            values = both_parts(spread_ref, pl.ds(place, half, stride=PITCH))
            rows = pl.ds(place, outer, stride=ODD)
            work[0, rows, :], work[1, rows, :] = combine(dot(outer_ref[place], values), False)
        return carry

    lax.fori_loop(0, inner // NEAR, forward, 0)
    for copy in copies(step_id):
        copy.wait()
    slot = step_id % 2

    def middle(step, carry):
        for index in range(NEAR):
            place = step * NEAR + index
            rows = pl.ds(place * ODD, inner)
            re, im = combine(dot(inner_ref[...], both_parts(work, rows)), False)
            psf_re = psf[slot, 0, :, place, :]
            psf_im = psf[slot, 1, :, place, :]
            values = jnp.concatenate(
                [re * psf_re - im * psf_im, re * psf_im + im * psf_re], axis=1
            )
            values = right_parts(values)
            work[0, rows, :], work[1, rows, :] = combine(dot(inner_ref[...], values), True)
        return carry

    lax.fori_loop(0, outer // NEAR, middle, 0)

    def backward(step, carry):
        for index in range(NEAR):
            place = step * NEAR + index
            values = both_parts(work, pl.ds(place, outer, stride=ODD))
            rows = pl.ds(place, half, stride=ODD)
            work[0, rows, :], work[1, rows, :] = combine(dot(back_ref[place], values), False)
        return carry

    lax.fori_loop(0, inner // NEAR, backward, 0)
    span = inner // pieces
    runs = half // (2 * owners)
    for out, held in zip(outs, plan):
        for owner in range(owners):
            for spot, (side, piece) in enumerate(held):
                for part in range(2):
                    for run in range(runs):
                        source = ((side * owners + owner) * runs + run) * ODD + piece * span
                        target = (((owner * len(held) + spot) * 2 + part) * runs + run) * span
                        out[target : target + span, :] = work[part, source : source + span, :]


def column_stage(spread, psf_re, psf_im, tables, plan, owners, pieces, first, count):
    height = spread.shape[1]
    width = height // PITCH * TILE_R
    outer = 2 * width // TILE_R
    outer_table, inner_table, back_table = tables
    sizes = [width // 2 // pieces * len(held) * 2 for held in plan]

    def fixed(table):
        zeros = (0,) * table.ndim
        return pl.BlockSpec(table.shape, lambda step: zeros, pipeline_mode=pl.Buffered(1))

    def body(*refs):
        column_kernel(plan, owners, pieces, first, *refs)

    def by_turn(psf):
        return psf.reshape(TILE_R, outer, psf.shape[2])

    return pl.pallas_call(
        body,
        out_shape=[jax.ShapeDtypeStruct((size, count * LANES), F32) for size in sizes],
        grid=(count,),
        in_specs=[
            pl.BlockSpec((2, height, LANES), lambda step: (0, 0, step)),
            pl.BlockSpec(memory_space=pl.ANY),
            pl.BlockSpec(memory_space=pl.ANY),
            fixed(outer_table),
            fixed(inner_table),
            fixed(back_table),
        ],
        out_specs=[pl.BlockSpec((size, LANES), lambda step: (0, step)) for size in sizes],
        scratch_shapes=[
            pltpu.VMEM((2, outer * ODD, LANES), F32),
            pltpu.VMEM((2, 2, TILE_R, outer + 8, LANES), F32),
            pltpu.SemaphoreType.DMA((2, 2)),
        ],
        compiler_params=params(),
        cost_estimate=cost(count * 2.5e10, count * 2e7),
    )(spread, by_turn(psf_re), by_turn(psf_im), outer_table, inner_table, back_table)


def column_tables(width, length, half_id):
    inner = TILE_R
    half = width // inner
    outer = 2 * half
    fast = jnp.arange(inner, dtype=jnp.int32)
    slow = jnp.arange(half, dtype=jnp.int32)
    freq = jnp.arange(outer, dtype=jnp.int32)
    coarse = unit(freq[:, None] * slow[None, :], outer, -1.0)
    fine = unit(fast[:, None] * freq[None, :], length, -1.0)
    cosine, sine = product([part[None] for part in coarse], [part[:, :, None] for part in fine])
    outer_table = left_parts(jnp.concatenate([cosine, sine], axis=1))
    cosine, sine = unit(fast[:, None] * fast[None, :], inner, -1.0)
    inner_table = left_parts(jnp.concatenate([cosine, sine], axis=0))
    count = inner // 2
    last_table = left_parts(jnp.concatenate([cosine[:count], sine[:count]], axis=0))
    ranks = (slow + half // 2 * (1 - half_id)) % half
    coarse = unit(ranks[:, None] * freq[None, :], outer, 1.0)
    fine = unit(fast[:, None] * freq[None, :], length, 1.0)
    cosine, sine = product([part[None] for part in coarse], [part[:, None, :] for part in fine])
    back_table = left_parts(jnp.concatenate([cosine, sine], axis=1))
    return (outer_table, inner_table, back_table), last_table


def last_kernel(groups, signs, outer_ref, last_ref, *rest):
    ins, rest = rest[:groups], rest[groups:]
    base, (out_ref, flat, work, image) = rest[:-4], rest[-4:]
    owners, _, _, rows, lanes = ins[0].shape
    inner = TILE_R
    chunks = lanes // LANES
    turns = LANES // inner
    if rows < LANES:
        flat[...] = jnp.zeros_like(flat)
    for owner in range(owners):
        for group in range(groups):
            for chunk in range(chunks):
                start = ((owner * groups + group) * chunks + chunk) * turns
                lane = chunk * LANES
                for part in range(2):
                    values = ins[group][owner, 0, part, :, lane : lane + LANES].T
                    for turn in range(turns):
                        place = (start + turn) * PITCH
                        flat[part, place : place + inner, :rows] = values[
                            turn * inner : (turn + 1) * inner
                        ]
    half = flat.shape[1] // PITCH
    outer = 2 * half

    def forward(step, carry):
        for index in range(8):
            place = step * 8 + index
            values = both_parts(flat, pl.ds(place, half, stride=PITCH))
            span = pl.ds(place, outer, stride=ODD)
            work[0, span, :], work[1, span, :] = combine(dot(outer_ref[place], values), True)
        return carry

    lax.fori_loop(0, inner // 8, forward, 0)
    count = last_ref.shape[0] // 2

    def final(step, carry):
        for index in range(8):
            place = step * 8 + index
            both = dot(last_ref[...], both_parts(work, pl.ds(place * ODD, inner)))
            re, _ = combine(both, True)
            image[pl.ds(place, count, stride=outer + 8), :] = re * signs[index % 2]
        return carry

    lax.fori_loop(0, outer // 8, final, 0)
    runs, _, span, width = out_ref.shape
    for tile in range(width // LANES):
        place = tile * LANES // outer * (outer + 8) + tile * LANES % outer
        values = image[place : place + LANES, :].T
        cols = slice(tile * LANES, (tile + 1) * LANES)
        for run in range(runs):
            part = values[run * span : (run + 1) * span]
            if base:
                part = base[0][run, 0, :, cols] - part
            out_ref[run, 0, :, cols] = part


def last_stage(parts, spots, steps, span, outer_table, last_table, signs, base=()):
    owners, _, _, rows, lanes = parts[0].shape
    groups = len(parts)
    step_rows = min(rows, LANES)
    per = rows // step_rows
    width = owners * groups * lanes
    runs = step_rows // span

    def fixed(table):
        zeros = (0,) * table.ndim
        return pl.BlockSpec(table.shape, lambda step, *_: zeros, pipeline_mode=pl.Buffered(1))

    def part_spec(spot):
        return pl.BlockSpec(
            (owners, 1, 2, step_rows, lanes),
            lambda step, *_: (0, spot + step // per, 0, step % per, 0),
        )

    natural = pl.BlockSpec((runs, 1, span, width), lambda step, *_: (step % per, step // per, 0, 0))

    def body(*refs):
        last_kernel(groups, *refs)

    outer = 2 * width // TILE_R
    return pl.pallas_call(
        body,
        out_shape=jax.ShapeDtypeStruct((rows // span, steps, span, width), F32),
        grid_spec=pltpu.PrefetchScalarGridSpec(
            num_scalar_prefetch=1,
            grid=(steps * per,),
            in_specs=[fixed(outer_table), fixed(last_table)]
            + [part_spec(spot) for spot in spots]
            + [natural] * len(base),
            out_specs=natural,
            scratch_shapes=[
                pltpu.VMEM((2, width // TILE_R * PITCH, LANES), F32),
                pltpu.VMEM((2, outer * ODD, LANES), F32),
                pltpu.VMEM((width // outer * (outer + 8), LANES), F32),
            ],
        ),
        compiler_params=params(),
        cost_estimate=cost(steps * rows * 8e7, steps * rows * 5e4),
    )(signs, outer_table, last_table, *parts, *base)


def finish_kernel(*refs):
    base_ref, others, (out_ref, sum_ref, top_ref) = refs[0], refs[1:-3], refs[-3:]

    @pl.when(pl.program_id(0) == 0)
    def _():
        sum_ref[...] = jnp.zeros_like(sum_ref)
        top_ref[...] = jnp.zeros_like(top_ref)

    total = sum_ref[...]
    top = top_ref[...]
    span, width = base_ref.shape[2:]
    for number, other in enumerate(others):
        values = base_ref[0, number] - other[0, 0]
        out_ref[0, number] = values
        sizes = (span // 8, 8, width)
        total = total + jnp.sum((values * values).reshape(sizes), axis=0)
        top = jnp.maximum(top, jnp.max(jnp.abs(values).reshape(sizes), axis=0))
    sum_ref[...] = total
    top_ref[...] = top


def finish(base, others):
    runs, pieces, span, width = base.shape
    whole = pl.BlockSpec((1, pieces, span, width), lambda step: (step, 0, 0, 0))
    one = pl.BlockSpec((1, 1, span, width), lambda step: (step, 0, 0, 0))
    small = pl.BlockSpec((8, width), lambda step: (0, 0))
    return pl.pallas_call(
        finish_kernel,
        out_shape=[
            jax.ShapeDtypeStruct(base.shape, F32),
            jax.ShapeDtypeStruct((8, width), F32),
            jax.ShapeDtypeStruct((8, width), F32),
        ],
        grid=(runs,),
        in_specs=[whole] + [one] * pieces,
        out_specs=[whole, small, small],
        compiler_params=params(),
        cost_estimate=cost(base.size * 4, base.size * 12),
    )(base, *others)


def on_device(flux, offsets, counts, dest_owner, dest_tile, dirty, psf_real, psf_imag):
    slab_count = lax.axis_size("slab")
    slab_id = lax.axis_index("slab")
    _, rows_dev, width = dirty.shape
    length = 2 * width
    blocks_dev, slots = offsets.shape
    blocks = blocks_dev * slab_count
    across = width // TILE_C
    col_count = psf_real.shape[2]
    chunks = col_count // LANES
    first_col = slab_id * col_count
    owners = slab_count // 2
    half_id = slab_id // owners
    halves = [list(range(owners)), list(range(owners, slab_count))]
    partners = [(i, (i + owners) % slab_count) for i in range(slab_count)]

    live_mask = jnp.arange(slots, dtype=jnp.int32)[None, :] < counts[:, None]
    weights = jnp.where(live_mask, flux[0], 0.0)
    tile_count = (rows_dev // TILE_R) * across
    places = dest_owner * tile_count + dest_tile[:, None]
    packed = jnp.stack(
        [weights, offsets.astype(F32), jnp.broadcast_to(places, offsets.shape).astype(F32)], axis=1
    )
    packed = lax.all_gather(packed, "slab", axis=0, tiled=True)
    amounts = packed[:, 0:1]
    points = packed[:, 1:2].astype(jnp.int32)
    places = packed[:, 2, 0].astype(jnp.int32)
    rows, cols = points // TILE_C, points % TILE_C
    bands, tile_cols = places // across, places % across

    pieces = max(1, min(2, rows_dev // LANES))
    part_rows = rows_dev // pieces
    tables, last_table = column_tables(width, length, half_id)
    groups = 4 if chunks % 4 == 0 else 1
    sparse = blocks * TILE_R <= 8 * width
    if sparse:
        tiles = make_tiles(rows, cols, amounts)
        basis, turns = row_tables(first_col, col_count, length, across)
    count = chunks // groups
    every = tuple(range(pieces))

    def swap(part):
        return lax.all_to_all(part, "slab", 0, 0, axis_index_groups=halves, tiled=True)

    far, near = [], []
    for group in range(groups):
        first = group * count
        if sparse:
            spread = row_transform(bands, tile_cols, tiles, basis, turns, width, first, count)
        else:
            spread = dense_rows(
                bands, tile_cols, rows, cols, amounts, width, first_col, col_count, length
            )
        last = group == groups - 1
        sides = [[(side, piece) for piece in every] for side in range(2)]
        if last:
            plan = [[held] for held in sides[0]] + [sides[1]]
        elif group == 0:
            plan = [sides[0] + sides[1]]
        else:
            plan = sides
        made = column_stage(spread, psf_real, psf_imag, tables, plan, owners, pieces, first, count)
        made = [
            part.reshape(owners, len(held), 2, part_rows, count * LANES)
            for part, held in zip(made, plan)
        ]
        bands, *made = lax.optimization_barrier((bands, *made))
        if len(plan) > 1:
            near.append(made.pop())
        far.append([swap(part) for part in made])
    scale = 1.0 / (length * length)
    odd = jnp.where(half_id == 0, scale, -scale)
    signs = jnp.stack([jnp.full_like(odd, scale), odd])
    span = TILE_R // pieces
    final = (tables[0], last_table, signs)
    others = []
    for piece in every:
        parts = [held[0] for held in far[:-1]] + [far[-1][piece]]
        spots = [piece] * (groups - 1) + [0]
        made = last_stage(parts, spots, 1, span, *final)
        others.append(lax.ppermute(made, "slab", partners))
    near = [swap(part) for part in near]
    near = [held[0] for held in far[: groups - len(near)]] + near
    base = dirty.reshape(rows_dev // TILE_R, pieces, span, width)
    spots = [pieces] + [0] * (groups - 1) if groups > 1 else [0]
    base = last_stage(near, spots, pieces, span, *final, (base,))
    residual, sums, tops = finish(base, others)
    residual = residual.reshape(1, rows_dev, width)
    stats = jnp.stack([jnp.sum(sums), jnp.max(tops)])
    stats = lax.all_gather(stats, "slab", axis=0, tiled=False)
    total = rows_dev * slab_count * width
    stats = jnp.stack([jnp.sqrt(jnp.sum(stats[:, 0]) / total), jnp.max(stats[:, 1])])
    stats = lax.all_gather(stats, "chan", axis=0, tiled=False)
    rms_values, peak_values = stats[:, 0], stats[:, 1]
    return (residual, rms_values, peak_values)


def solution(mesh):
    placed = (
        P("chan", "slab", None),
        P("slab", None),
        P("slab"),
        P("slab", None),
        P("slab"),
        P("chan", "slab", None),
        P("chan", None, "slab"),
        P("chan", None, "slab"),
    )
    return jax.shard_map(
        on_device,
        mesh=mesh,
        in_specs=placed,
        out_specs=(P("chan", "slab", None), P(), P()),
        check_vma=False,
    )
```
